32 devices in a mesh: gx: 4 (over x, core), gy: 4 (over z), gz: 2 (over y).
Axes of the slice: x: 2, y: 2, z: 4, core: 2. Of those that a mesh axis runs over, the one named last changes fastest.
Arguments:
- grad_bucket: bfloat16 [32, 1, 3584, 1024], P(('gx', 'gy', 'gz')), may hold values from -72000 to 72000
- parameters: bfloat16 [1, 3584, 1024], P(None, ('gx', 'gy', 'gz')), may hold values from -4 to 4
- row_state: float32 [1, 3584], P(None, ('gx', 'gy', 'gz')), may hold values from 0.01 to 10
- column_state: float32 [1, 1024], replicated, may hold values from 0.01 to 10
Outputs:
- new_parameters: bfloat16 [1, 3584, 1024], P(None, ('gx', 'gy', 'gz'))
- row_next: float32 [1, 3584], P(None, ('gx', 'gy', 'gz'))
- column_next: float32 [1, 1024], replicated
- first_layer: bfloat16 [3584, 1024], replicated
The draws below stay inside these ranges and needn't reach their ends.
All inputs are finite; a program needn't handle non-finite values.
Results may differ from the reference program's by a relative error of at most 0.011.
Values may be sent and summed in bfloat16 or wider, within the bound.
No kernel may reach another device: no remote copies, remote signals or barrier semaphores. Data moves between devices by JAX's collectives and lax.ppermute only.
A program may use at most 128 MiB of HBM per device.

```python
import math
import jax
import jax.numpy as jnp
from jax import lax

D = 3584
LAYERS = 1
KW = 1024
DEVICES = 32


def draw_grad_bucket(key, part):
    row_key = jax.random.fold_in(key, 11)
    column_key = jax.random.fold_in(key, 12)
    owner_key = jax.random.fold_in(key, 13)
    row_index = jnp.arange(D, dtype=jnp.int32)
    rising = jnp.exp(math.log(3.0) * row_index.astype(jnp.float32) / (D - 1))
    row_scale = rising[None, :] * jnp.exp(math.log(10.0) * jax.random.uniform(row_key, (LAYERS, D)))
    column_scale = jnp.exp(math.log(10.0) * jax.random.uniform(column_key, (LAYERS, KW)))
    owners = jax.random.permutation(owner_key, DEVICES).astype(jnp.int32)
    row_owner = row_index // (D // DEVICES)

    def one_device(device):
        device_key = jax.random.fold_in(key, 1000 + device)
        noise_part = jnp.clip(jax.random.normal(device_key, (LAYERS, D, KW)), -6.0, 6.0)
        spiked = jnp.where(row_owner == owners[device], 24.0, 1.0)
        values = noise_part * row_scale[:, :, None] * column_scale[:, None, :] * spiked[None, :, None]
        return values.astype(jnp.bfloat16)
    return lax.map(one_device, jnp.arange(DEVICES, dtype=jnp.int32))


def steps_of(rng, dims, pieces, low, high):
    loudness, own = 1.0, jax.random.fold_in(rng, 6)
    for axis_at, shards_of in pieces:
        steps = jnp.exp(jax.random.uniform(jax.random.fold_in(own, axis_at), (shards_of,), jnp.float32, low / len(pieces), high / len(pieces)))
        loudness = loudness * jnp.repeat(steps, dims[axis_at] // shards_of).reshape([-1 if axis == axis_at else 1 for axis in range(len(dims))])
    return loudness


def normal_values(stream_key, extent, scale, most, shards=(), kind=jnp.bfloat16):
    array = scale * jax.random.normal(stream_key, extent, jnp.float32)
    if shards:
        array = array * steps_of(stream_key, extent, shards, -0.22, 0.18)
    return jnp.clip(array, -most, most).astype(kind)


def setup_inputs(seed: int = 0) -> dict:
    key_of = jax.random.split(jax.random.key(seed), 5)
    grad_bucket = draw_grad_bucket(jax.random.fold_in(key_of[4], 71), 0)
    parameters = normal_values(key_of[1], (LAYERS, D, KW), 1.0, 4.0, ((1, 32),))
    row_state = jnp.clip(jnp.exp(math.log(10.0) - 6.9077553 * jax.random.uniform(key_of[2], (LAYERS, D), jnp.float32) ** steps_of(key_of[2], (LAYERS, D), ((1, 32),), -0.2, 0.2)), 0.01, 10.0)
    column_state = jnp.clip(jnp.exp(jax.random.uniform(key_of[3], (LAYERS, KW), jnp.float32, math.log(0.01), math.log(10.0))), 0.01, 10.0)
    return dict(grad_bucket=grad_bucket, parameters=parameters, row_state=row_state, column_state=column_state)


beta_two = 0.8
step_size = 0.5

def reference(grad_bucket, parameters, row_state, column_state):

    def accumulate(running, device_grad):
        return (running + device_grad.astype(jnp.float32), None)
    summed, unused = lax.scan(accumulate, jnp.zeros((LAYERS, D, KW), jnp.float32), grad_bucket)
    norm_square = jnp.sum(summed * summed)
    clip_level = 0.5 * math.sqrt(LAYERS * D * KW)
    factor = jnp.minimum(jnp.float32(1.0), clip_level / jnp.sqrt(norm_square + 1e-06))
    clipped = factor * summed
    squares = clipped * clipped
    row_next = beta_two * row_state + (1.0 - beta_two) * lax.optimization_barrier(jnp.mean(squares, axis=2))
    column_next = beta_two * column_state + (1.0 - beta_two) * lax.optimization_barrier(jnp.mean(squares, axis=1))
    row_average = lax.optimization_barrier(jnp.mean(row_next, axis=1))
    second = row_next[:, :, None] * column_next[:, None, :] / row_average[:, None, None]
    update = clipped / jnp.sqrt(second)
    new_parameters = (parameters.astype(jnp.float32) - step_size * update).astype(jnp.bfloat16)
    return (new_parameters, row_next, column_next, new_parameters[0])
```

```python
import math

import jax
import jax.numpy as jnp
from jax import lax
from jax.sharding import PartitionSpec as P

beta_two = 0.8
step_size = 0.5


class Plan:
    def __init__(self, mesh):
        self.axes = tuple(mesh.axis_names)
        self.count = math.prod(mesh.shape[a] for a in self.axes)
        self.bits = []
        for a in self.axes:
            width = mesh.shape[a].bit_length() - 1
            assert 1 << width == mesh.shape[a]
            self.bits += [(a, b) for b in reversed(range(width))]
        first, middle, last = self.axes
        chip = self.bits.index((first, 0))
        lead = [self.bits.index((first, 1)), self.bits.index((last, 0)), self.bits.index((middle, 0))]
        rest = [d for d in range(len(self.bits)) if d != chip and d not in lead]
        self.chip = chip
        self.orders = [[chip] + lead[i:] + lead[:i] + rest[::-1] for i in range(len(lead))]

    def mine(self, d):
        a, b = self.bits[d]
        return (lax.axis_index(a) >> b) & 1

    def swap(self, value, d):
        flip = 1 << (len(self.bits) - 1 - d)
        return lax.ppermute(value, self.axes, [(i, i ^ flip) for i in range(self.count)])


def pick(value, d, at):
    return lax.dynamic_index_in_dim(value, at, axis=d, keepdims=True)


def scatter_sum(plan, grid, order):
    first = order[0]
    send = pick(grid, first, 1 - plan.mine(first))
    keep = pick(grid, first, plan.mine(first))
    for at, d in enumerate(order):
        got = plan.swap(send, d)
        if at + 1 == len(order):
            return keep.astype(jnp.float32) + got.astype(jnp.float32)
        n = order[at + 1]

        def part(which):
            whole = pick(keep, n, which).astype(jnp.float32) + pick(got, n, which).astype(jnp.float32)
            return whole.astype(jnp.bfloat16)

        send, keep = part(1 - plan.mine(n)), part(plan.mine(n))


def gather(plan, block, order):
    for d in reversed(order):
        got = plan.swap(block, d)
        low = plan.mine(d) == 0
        block = jnp.concatenate([jnp.where(low, block, got), jnp.where(low, got, block)], axis=d)
    return block


def all_sum(plan, value):
    for d in plan.orders[0]:
        value = value + plan.swap(value, d)
    return value


def make(mesh):
    plan = Plan(mesh)

    def shards(grad_bucket, parameters, row_state, column_state):
        _, layers, width, columns = grad_bucket.shape
        rows = width // plan.count
        lanes = 128
        tiles = columns // lanes
        colours = len(plan.orders)
        edges = [lanes * (-(-tiles * i // colours)) for i in range(colours + 1)]
        spans = list(zip(edges[:-1], edges[1:]))
        ones = [2] * len(plan.bits)
        grid = grad_bucket.reshape(ones + [rows, columns])
        summed = []
        for order, (lo, hi) in zip(plan.orders, spans):
            summed.append(scatter_sum(plan, grid[..., lo:hi], order).reshape(rows, hi - lo))

        square_rows = sum(jnp.sum(s * s, axis=1) for s in summed)
        square_columns = [jnp.sum(s * s, axis=0) for s in summed]
        state_total = jnp.broadcast_to(jnp.sum(row_state), (lanes,))
        packed = jnp.concatenate(square_columns + [state_total]).reshape(-1, lanes)
        packed = all_sum(plan, packed).reshape(-1)
        square_columns, state_total = packed[:columns], packed[columns]
        norm_square = jnp.sum(square_columns)
        clip_level = 0.5 * math.sqrt(layers * width * columns)
        factor = jnp.minimum(jnp.float32(1.0), clip_level / jnp.sqrt(norm_square + 1e-06))
        scale = factor * factor
        row_next = beta_two * row_state[0] + (1.0 - beta_two) * (scale * square_rows / columns)
        column_next = beta_two * column_state[0] + (1.0 - beta_two) * (scale * square_columns / width)
        row_average = (beta_two * state_total + (1.0 - beta_two) * (scale * norm_square / columns)) / width
        row_factor = step_size * factor * lax.rsqrt(row_next / row_average)
        column_factor = lax.rsqrt(column_next)

        fresh, whole = [], []
        for order, (lo, hi), s in zip(plan.orders, spans, summed):
            update = s * row_factor[:, None] * column_factor[None, lo:hi]
            new = (parameters[0, :, lo:hi].astype(jnp.float32) - update).astype(jnp.bfloat16)
            fresh.append(new)
            block = new.reshape([1] * len(plan.bits) + [rows, hi - lo])
            whole.append(gather(plan, block, order).reshape(width, hi - lo))
        new_parameters = jnp.concatenate(fresh, axis=1)[None]
        first_layer = jnp.concatenate(whole, axis=1)
        return new_parameters, row_next[None], column_next[None], first_layer

    return shards


def solution(mesh):
    in_specs = (
        P(("gx", "gy", "gz"), None, None, None),
        P(None, ("gx", "gy", "gz"), None),
        P(None, ("gx", "gy", "gz")),
        P(),
    )
    out_specs = (P(None, ("gx", "gy", "gz"), None), P(None, ("gx", "gy", "gz")), P(), P())
    return jax.shard_map(make(mesh), mesh=mesh, in_specs=in_specs, out_specs=out_specs, check_vma=False)
```
